512 devices in a mesh: tm: 8 (over y_lo, x), band: 64 (over z, y_hi, core).
Axes of the slice: x: 4, y: 4 (y_hi: 2, y_lo: 2; y = y_hi * 2 + y_lo), z: 16, core: 2. Of those that a mesh axis runs over, the one named last changes fastest.
Arguments:
- samples: bfloat16 [2048, 256, 2, 512], P('tm', 'band'), may hold values from -6 to 6
- weights: bfloat16 [256, 2, 512, 512], P('band', None, None, 'tm'), may hold values from -0.25 to 0.25
- prototype: float32 [1024], replicated, may hold values from 0.25 to 1
Outputs:
- beam_series: float32 [512, 524288], P('band', 'tm')
The draws below stay inside these ranges and needn't reach their ends.
All inputs are finite; a program needn't handle non-finite values.
Results may differ from the reference program's by a relative error of at most 0.004.
Values may be sent and summed in bfloat16 or wider, within the bound.
No kernel may reach another device: no remote copies, remote signals or barrier semaphores. Data moves between devices by JAX's collectives and lax.ppermute only.
A program may use at most 128 MiB of HBM per device.

```python
import math
import jax
import jax.numpy as jnp
from jax import lax

M = 512
K = 256
FIRST_BIN = 32
E = 512
B = 512
L = 1024
NF = 2048


def steps_of(own_key, dims, cuts, least, top_value):
    gain = 1.0
    for axis_at, parts in cuts:
        draws = jax.random.uniform(jax.random.fold_in(jax.random.fold_in(own_key, 6), axis_at), (parts,), jnp.float32, least / len(cuts), top_value / len(cuts))
        gain = gain * jnp.repeat(jnp.exp(draws), dims[axis_at] // parts).reshape((-1,) + (1,) * (len(dims) - 1 - axis_at))
    return gain


def gaussian(rng, extent, scale, reach, shards=(), kind=jnp.bfloat16):
    level = steps_of(rng, extent, shards, -0.22, 0.18) if shards else 1.0
    array = jax.random.normal(rng, extent, jnp.float32) * scale * level
    return jnp.minimum(jnp.maximum(array, -reach), reach).astype(kind)


def setup_inputs(seed: int = 0) -> dict:
    key_of = jax.random.split(jax.random.key(seed), 4)
    return {
        "samples": gaussian(key_of[0], (NF, K, 2, E), 1.0, 6.0, ((0, 8), (1, 64))),
        "weights": gaussian(key_of[1], (K, 2, E, B), E ** -0.5, 0.25, ((0, 64), (3, 8))),
        "prototype": jnp.clip(jax.random.uniform(key_of[2], (L,), jnp.float32, 0.25, 1.0), 0.25, 1.0),
    }


def synth_table(prototype):
    length = prototype.shape[0]
    bin_index = jnp.arange(K, dtype=jnp.int32) + FIRST_BIN
    tap_index = jnp.arange(length, dtype=jnp.int32)
    phase_index = bin_index[:, None] * tap_index[None, :] % M
    angles = phase_index.astype(jnp.float32) * (2.0 * math.pi / M)
    scaled = prototype.astype(jnp.float32)[None, :] / math.sqrt(K)
    window_table = jnp.stack([jnp.cos(angles) * scaled, -jnp.sin(angles) * scaled], axis=1)
    return window_table.astype(jnp.bfloat16)

def intersection_add(frames, hop_size):
    pieces = frames.shape[-1] // hop_size
    pieces_view = frames.reshape(frames.shape[:-1] + (pieces, hop_size))
    leading = [(0, 0)] * (pieces_view.ndim - 3)
    intersection = jnp.zeros(pieces_view.shape[:-3] + (pieces_view.shape[-3] + pieces - 1, hop_size), frames.dtype)
    for lag in range(pieces):
        intersection = intersection + jnp.pad(pieces_view[..., lag, :], leading + [(lag, pieces - 1 - lag), (0, 0)])
    return intersection

def reference(samples, weights, prototype):
    hop_size = M // 2
    frame_total = samples.shape[0]

    def form_bin(operands):
        bin_samples, bin_weights = operands
        products = jnp.einsum('fce,deb->bdcf', bin_samples.astype(jnp.float32), bin_weights.astype(jnp.float32), precision=lax.Precision.HIGHEST)
        real_part = products[:, 0, 0] + products[:, 1, 1]
        imag_part = products[:, 0, 1] - products[:, 1, 0]
        return jnp.stack([real_part, imag_part], axis=1).astype(jnp.bfloat16)
    spectra = lax.map(form_bin, (jnp.moveaxis(samples, 1, 0), weights))
    window_table = synth_table(prototype).astype(jnp.float32)

    def synth_beam(beam_spectra):
        frame_out = jnp.einsum('kcf,kcn->fn', beam_spectra.astype(jnp.float32), window_table, precision=lax.Precision.HIGHEST)
        summed = intersection_add(frame_out, hop_size)
        return summed[:frame_total].reshape(frame_total * hop_size)
    return lax.map(synth_beam, jnp.moveaxis(spectra, 1, 0))
```

```python
import math

import jax
import jax.numpy as jnp
from jax import lax
from jax.experimental import pallas as pl
from jax.experimental.pallas import tpu as pltpu
from jax.sharding import PartitionSpec as P


M = 512
K = 256
FIRST_BIN = 32
LANES = 128
HEAD = 1


def passed_along(block, axis, distance):
    devices = range(lax.axis_size(axis))
    route = [(i - distance, i) for i in devices if i - distance in devices]
    return lax.ppermute(block, axis, route)


def synth_table(prototype):
    length = prototype.shape[0]
    bin_index = jnp.arange(K, dtype=jnp.int32) + FIRST_BIN
    tap_index = jnp.arange(length, dtype=jnp.int32)
    phase_index = bin_index[:, None] * tap_index[None, :] % M
    angles = phase_index.astype(jnp.float32) * (2.0 * math.pi / M)
    scaled = prototype[None, :] / math.sqrt(K)
    window_table = jnp.stack([jnp.cos(angles) * scaled, -jnp.sin(angles) * scaled], axis=1)
    return window_table.astype(jnp.bfloat16)


def intersection_add(frames, hop_size):
    pieces = frames.shape[-1] // hop_size
    pieces_view = frames.reshape(frames.shape[:-1] + (pieces, hop_size))
    leading = [(0, 0)] * (pieces_view.ndim - 3)
    intersection = jnp.zeros(
        pieces_view.shape[:-3] + (pieces_view.shape[-3] + pieces - 1, hop_size), frames.dtype
    )
    for lag in range(pieces):
        intersection = intersection + jnp.pad(
            pieces_view[..., lag, :], leading + [(lag, pieces - 1 - lag), (0, 0)]
        )
    return intersection


def overlap_kernel(frames_ref, base_ref, out_ref):
    beams, rows, hop_size = base_ref.shape
    lags = frames_ref.shape[2] // hop_size
    step, lanes = 32, out_ref.shape[1]
    halves = hop_size // lanes

    def one_beam(b, carry):
        for at in range(0, rows, step):
            total = base_ref[b, pl.ds(at, step), :] + frames_ref[b, pl.ds(at, step), :hop_size]
            for lag in range(1, lags):
                columns = pl.ds(lag * hop_size, hop_size)
                if at:
                    total += frames_ref[b, pl.ds(at - lag, step), columns]
                else:
                    piece = pltpu.roll(frames_ref[b, pl.ds(0, step), columns], lag, 0)
                    row = lax.broadcasted_iota(jnp.int32, piece.shape, 0)
                    total += jnp.where(row < lag, 0.0, piece)
            for half in range(halves):
                rows_of = pl.ds((at * halves + half) * beams + b, step, stride=halves * beams)
                out_ref[rows_of, :] = total[:, half * lanes : (half + 1) * lanes]
        return carry

    lax.fori_loop(0, beams, one_beam, 0)


def overlapped(frames, base):
    beams, rows, hop_size = base.shape
    lags = frames.shape[2] // hop_size
    whole = pl.BlockSpec(memory_space=pltpu.VMEM)
    return pl.pallas_call(
        overlap_kernel,
        out_shape=jax.ShapeDtypeStruct((rows * hop_size // LANES * beams, LANES), jnp.float32),
        in_specs=[whole, whole],
        out_specs=whole,
        cost_estimate=pl.CostEstimate(
            flops=beams * lags * rows * hop_size,
            bytes_accessed=4 * beams * (lags + 2) * rows * hop_size,
            transcendentals=0,
        ),
        compiler_params=pltpu.CompilerParams(vmem_limit_bytes=20 * 2**20),
        name="overlap",
    )(frames, base)


def exchanged(block, axis):
    return lax.all_to_all(block, axis, split_axis=0, concat_axis=0, tiled=True)


def gathered_by_permutes(block):
    size = lax.axis_size("tm")
    ring = size // 2

    def moved(array, x_step, y_step):
        route = [
            (i, ((i // ring + y_step) % 2) * ring + (i % ring + x_step) % ring)
            for i in range(size)
        ]
        return lax.ppermute(array, "tm", route)

    half = block.shape[-2] // 2
    left = moved(block, 1, 0)
    right = moved(block, -1, 0)
    across = moved(block, 0, 1)
    far_a = moved(left[..., :half, :], 1, 0)
    far_b = moved(right[..., half:, :], -1, 0)
    across_left = moved(across, 1, 0)
    across_right = moved(across, -1, 0)
    across_far = moved(block, 2, 1)
    far = jnp.concatenate([far_a, far_b], axis=-2)
    me = lax.axis_index("tm")
    y, x = me // ring, me % ring
    table = jnp.zeros((size,) + block.shape, block.dtype)
    for piece, dx, dy in (
        (block, 0, 0), (left, -1, 0), (right, 1, 0), (far, 2, 0),
        (across, 0, 1), (across_left, -1, 1), (across_right, 1, 1), (across_far, 2, 1),
    ):
        at = ((y + dy) % 2) * ring + (x + dx + ring) % ring
        table = lax.dynamic_update_slice(table, piece[None], (at,) + (0,) * block.ndim)
    return table


def beam_form(samples, weights):
    products = jnp.einsum(
        "pfkce,tkcbe->tbkpf", samples, weights, preferred_element_type=jnp.float32
    )
    spectra = products.astype(jnp.bfloat16)
    size = lax.axis_size("band")
    spectra = spectra.reshape((size, -1) + spectra.shape[2:])
    return jnp.transpose(spectra, (0, 2, 3, 1, 4))


def shards(samples, weights, prototype):
    hop_size = M // 2
    blocks = jnp.transpose(weights, (0, 1, 3, 2))
    size = lax.axis_size("tm")
    head = blocks[:HEAD]
    head = exchanged(jnp.broadcast_to(head[None], (size,) + head.shape), "tm")
    both = jnp.stack([samples, jnp.stack([samples[:, :, 1], -samples[:, :, 0]], axis=2)])
    head_spectra = exchanged(beam_form(both[:, :, :HEAD], head), "band")
    rest = gathered_by_permutes(blocks[HEAD:])
    rest_spectra = exchanged(beam_form(both[:, :, HEAD:], rest), "band")

    table = synth_table(prototype)
    table = table.reshape((lax.axis_size("band"), -1) + table.shape[1:])

    frame_total = samples.shape[0]
    beams = head_spectra.shape[3]
    lags = prototype.shape[0] // hop_size

    def synthesize(spectra, part):
        return jnp.einsum(
            "skcbf,skcm->bfm", spectra, part, preferred_element_type=jnp.float32
        )

    def spill_of(tail):
        tail = tail.reshape(beams, lags - 1, lags, hop_size)
        rows = []
        for row in range(lags - 1):
            rows.append(
                sum(tail[:, lags - 1 + row - lag, lag] for lag in range(row + 1, lags))
            )
        return jnp.stack(rows)

    base = intersection_add(synthesize(head_spectra, table[:, :HEAD]), hop_size)
    base, spill = base[:, :frame_total], base[:, frame_total:]
    base, spill, rest_spectra = lax.optimization_barrier((base, spill, rest_spectra))
    rest_frames = synthesize(rest_spectra, table[:, HEAD:])
    spill = spill_of(rest_frames[:, frame_total - lags + 1 :]) + jnp.transpose(spill, (1, 0, 2))
    spill = spill.reshape(lags - 1, beams, -1, LANES)
    spill = jnp.transpose(spill, (0, 2, 1, 3)).reshape(-1, LANES)
    prev_tail = passed_along(spill, "tm", 1)
    out = overlapped(rest_frames, base)
    out = lax.dynamic_update_slice(out, out[: prev_tail.shape[0]] + prev_tail, (0, 0))
    out = out.reshape(-1, beams, LANES)
    return jnp.transpose(out, (1, 0, 2)).reshape(beams, frame_total * hop_size)


def solution(mesh):
    in_specs = (P("tm", "band", None, None), P("band", None, None, "tm"), P())
    out_specs = P("band", "tm")

    return jax.shard_map(shards, mesh=mesh, in_specs=in_specs, out_specs=out_specs, check_vma=False)
```

```python
import math

import jax
import jax.numpy as jnp
from jax import lax
from jax.experimental import pallas as pl
from jax.experimental.pallas import tpu as pltpu
from jax.sharding import PartitionSpec as P


M = 512
K = 256
FIRST_BIN = 32
LANES = 128
HEAD = 1


def passed_along(block, axis, distance):
    devices = range(lax.axis_size(axis))
    route = [(i - distance, i) for i in devices if i - distance in devices]
    return lax.ppermute(block, axis, route)


def synth_table(prototype):
    length = prototype.shape[0]
    bin_index = jnp.arange(K, dtype=jnp.int32) + FIRST_BIN
    tap_index = jnp.arange(length, dtype=jnp.int32)
    phase_index = bin_index[:, None] * tap_index[None, :] % M
    angles = phase_index.astype(jnp.float32) * (2.0 * math.pi / M)
    scaled = prototype[None, :] / math.sqrt(K)
    window_table = jnp.stack([jnp.cos(angles) * scaled, -jnp.sin(angles) * scaled], axis=1)
    return window_table.astype(jnp.bfloat16)


def intersection_add(frames, hop_size):
    pieces = frames.shape[-1] // hop_size
    pieces_view = frames.reshape(frames.shape[:-1] + (pieces, hop_size))
    leading = [(0, 0)] * (pieces_view.ndim - 3)
    intersection = jnp.zeros(
        pieces_view.shape[:-3] + (pieces_view.shape[-3] + pieces - 1, hop_size), frames.dtype
    )
    for lag in range(pieces):
        intersection = intersection + jnp.pad(
            pieces_view[..., lag, :], leading + [(lag, pieces - 1 - lag), (0, 0)]
        )
    return intersection


def overlap_kernel(frames_ref, base_ref, out_ref):
    beams, rows, hop_size = base_ref.shape
    lags = frames_ref.shape[2] // hop_size
    step, lanes = 32, out_ref.shape[1]
    halves = hop_size // lanes

    def one_beam(b, carry):
        for at in range(0, rows, step):
            total = base_ref[b, pl.ds(at, step), :] + frames_ref[b, pl.ds(at, step), :hop_size]
            for lag in range(1, lags):
                columns = pl.ds(lag * hop_size, hop_size)
                if at:
                    total += frames_ref[b, pl.ds(at - lag, step), columns]
                else:
                    piece = pltpu.roll(frames_ref[b, pl.ds(0, step), columns], lag, 0)
                    row = lax.broadcasted_iota(jnp.int32, piece.shape, 0)
                    total += jnp.where(row < lag, 0.0, piece)
            for half in range(halves):
                rows_of = pl.ds((at * halves + half) * beams + b, step, stride=halves * beams)
                out_ref[rows_of, :] = total[:, half * lanes : (half + 1) * lanes]
        return carry

    lax.fori_loop(0, beams, one_beam, 0)


def overlapped(frames, base):
    beams, rows, hop_size = base.shape
    lags = frames.shape[2] // hop_size
    whole = pl.BlockSpec(memory_space=pltpu.VMEM)
    return pl.pallas_call(
        overlap_kernel,
        out_shape=jax.ShapeDtypeStruct((rows * hop_size // LANES * beams, LANES), jnp.float32),
        in_specs=[whole, whole],
        out_specs=whole,
        cost_estimate=pl.CostEstimate(
            flops=beams * lags * rows * hop_size,
            bytes_accessed=4 * beams * (lags + 2) * rows * hop_size,
            transcendentals=0,
        ),
        compiler_params=pltpu.CompilerParams(vmem_limit_bytes=20 * 2**20),
        name="overlap",
    )(frames, base)


def exchanged(block, axis):
    return lax.all_to_all(block, axis, split_axis=0, concat_axis=0, tiled=True)


def across_tm(array, x_step, y_step):
    size = lax.axis_size("tm")
    ring = size // 2
    route = [
        (i, ((i // ring + y_step) % 2) * ring + (i % ring + x_step) % ring) for i in range(size)
    ]
    return lax.ppermute(array, "tm", route)


def own_row(block):
    return (
        across_tm(block, 1, 0),
        across_tm(block, -1, 0),
        across_tm(block, 0, 1),
        across_tm(block, 2, 0),
    )


def whole_table(block, left, right, across, far):
    across_left = across_tm(across, 1, 0)
    across_right = across_tm(across, -1, 0)
    across_far = across_tm(far, 0, 1)
    size = lax.axis_size("tm")
    ring = size // 2
    me = lax.axis_index("tm")
    y, x = me // ring, me % ring
    table = jnp.broadcast_to(block[None], (size,) + block.shape)
    for piece, dx, dy in (
        (left, -1, 0), (right, 1, 0), (across, 0, 1), (far, 2, 0),
        (across_left, -1, 1), (across_right, 1, 1), (across_far, 2, 1),
    ):
        at = ((y + dy) % 2) * ring + (x + dx + ring) % ring
        table = lax.dynamic_update_slice(table, piece[None], (at,) + (0,) * block.ndim)
    return table


def with_quadrature(samples):
    return jnp.stack([samples, jnp.stack([samples[:, :, 1], -samples[:, :, 0]], axis=2)])


def beam_form(samples, weights):
    products = jnp.einsum(
        "pfkce,tkcbe->tbkpf", samples, weights, preferred_element_type=jnp.float32
    )
    spectra = products.astype(jnp.bfloat16)
    size = lax.axis_size("band")
    spectra = spectra.reshape((size, -1) + spectra.shape[2:])
    return jnp.transpose(spectra, (0, 2, 3, 1, 4))


def shards(samples, weights, prototype):
    hop_size = M // 2
    blocks = jnp.transpose(weights, (0, 1, 3, 2))
    size = lax.axis_size("tm")
    head = blocks[:HEAD]
    head = exchanged(jnp.broadcast_to(head[None], (size,) + head.shape), "tm")
    row = own_row(blocks[HEAD:])
    message = beam_form(with_quadrature(samples[:, :HEAD]), head)
    head_spectra = exchanged(message, "band")
    samples, row, block, _ = lax.optimization_barrier((samples, row, blocks[HEAD:], message))
    rest = whole_table(block, *row)
    rest_spectra = exchanged(beam_form(with_quadrature(samples[:, HEAD:]), rest), "band")

    table = synth_table(prototype)
    table = table.reshape((lax.axis_size("band"), -1) + table.shape[1:])

    frame_total = samples.shape[0]
    beams = head_spectra.shape[3]
    lags = prototype.shape[0] // hop_size

    def synthesize(spectra, part):
        return jnp.einsum(
            "skcbf,skcm->bfm", spectra, part, preferred_element_type=jnp.float32
        )

    def spill_of(tail):
        tail = tail.reshape(beams, lags - 1, lags, hop_size)
        rows = []
        for row in range(lags - 1):
            rows.append(
                sum(tail[:, lags - 1 + row - lag, lag] for lag in range(row + 1, lags))
            )
        return jnp.stack(rows)

    base = intersection_add(synthesize(head_spectra, table[:, :HEAD]), hop_size)
    base, spill = base[:, :frame_total], base[:, frame_total:]
    base, spill, rest_spectra = lax.optimization_barrier((base, spill, rest_spectra))
    rest_frames = synthesize(rest_spectra, table[:, HEAD:])
    spill = spill_of(rest_frames[:, frame_total - lags + 1 :]) + jnp.transpose(spill, (1, 0, 2))
    spill = spill.reshape(lags - 1, beams, -1, LANES)
    spill = jnp.transpose(spill, (0, 2, 1, 3)).reshape(-1, LANES)
    prev_tail = passed_along(spill, "tm", 1)
    out = overlapped(rest_frames, base)
    out = lax.dynamic_update_slice(out, out[: prev_tail.shape[0]] + prev_tail, (0, 0))
    out = out.reshape(-1, beams, LANES)
    return jnp.transpose(out, (1, 0, 2)).reshape(beams, frame_total * hop_size)


def solution(mesh):
    in_specs = (P("tm", "band", None, None), P("band", None, None, "tm"), P())
    out_specs = P("band", "tm")

    return jax.shard_map(shards, mesh=mesh, in_specs=in_specs, out_specs=out_specs, check_vma=False)
```

```python
import math

import jax
import jax.numpy as jnp
from jax import lax
from jax.experimental import pallas as pl
from jax.experimental.pallas import tpu as pltpu
from jax.sharding import PartitionSpec as P


M = 512
K = 256
FIRST_BIN = 32
LANES = 128
PLANE = 4
HEAD = 1


def passed_along(block, axis, distance):
    devices = range(lax.axis_size(axis))
    route = [(i - distance, i) for i in devices if i - distance in devices]
    return lax.ppermute(block, axis, route)


def synth_table(prototype):
    length = prototype.shape[0]
    bin_index = jnp.arange(K, dtype=jnp.int32) + FIRST_BIN
    tap_index = jnp.arange(length, dtype=jnp.int32)
    phase_index = bin_index[:, None] * tap_index[None, :] % M
    angles = phase_index.astype(jnp.float32) * (2.0 * math.pi / M)
    scaled = prototype[None, :] / math.sqrt(K)
    window_table = jnp.stack([jnp.cos(angles) * scaled, -jnp.sin(angles) * scaled], axis=1)
    return window_table.astype(jnp.bfloat16)


def intersection_add(frames, hop_size):
    pieces = frames.shape[-1] // hop_size
    pieces_view = frames.reshape(frames.shape[:-1] + (pieces, hop_size))
    leading = [(0, 0)] * (pieces_view.ndim - 3)
    intersection = jnp.zeros(
        pieces_view.shape[:-3] + (pieces_view.shape[-3] + pieces - 1, hop_size), frames.dtype
    )
    for lag in range(pieces):
        intersection = intersection + jnp.pad(
            pieces_view[..., lag, :], leading + [(lag, pieces - 1 - lag), (0, 0)]
        )
    return intersection


def overlap_kernel(frames_ref, base_ref, out_ref):
    beams, rows, hop_size = base_ref.shape
    lags = frames_ref.shape[2] // hop_size
    step, lanes = 32, out_ref.shape[1]
    halves = hop_size // lanes

    def one_beam(b, carry):
        for at in range(0, rows, step):
            total = base_ref[b, pl.ds(at, step), :] + frames_ref[b, pl.ds(at, step), :hop_size]
            for lag in range(1, lags):
                columns = pl.ds(lag * hop_size, hop_size)
                if at:
                    total += frames_ref[b, pl.ds(at - lag, step), columns]
                else:
                    piece = pltpu.roll(frames_ref[b, pl.ds(0, step), columns], lag, 0)
                    row = lax.broadcasted_iota(jnp.int32, piece.shape, 0)
                    total += jnp.where(row < lag, 0.0, piece)
            for half in range(halves):
                rows_of = pl.ds((at * halves + half) * beams + b, step, stride=halves * beams)
                out_ref[rows_of, :] = total[:, half * lanes : (half + 1) * lanes]
        return carry

    lax.fori_loop(0, beams, one_beam, 0)


def overlapped(frames, base):
    beams, rows, hop_size = base.shape
    lags = frames.shape[2] // hop_size
    whole = pl.BlockSpec(memory_space=pltpu.VMEM)
    return pl.pallas_call(
        overlap_kernel,
        out_shape=jax.ShapeDtypeStruct((rows * hop_size // LANES * beams, LANES), jnp.float32),
        in_specs=[whole, whole],
        out_specs=whole,
        cost_estimate=pl.CostEstimate(
            flops=beams * lags * rows * hop_size,
            bytes_accessed=4 * beams * (lags + 2) * rows * hop_size,
            transcendentals=0,
        ),
        compiler_params=pltpu.CompilerParams(vmem_limit_bytes=20 * 2**20),
        name="overlap",
    )(frames, base)


def exchanged(block, axis):
    return lax.all_to_all(block, axis, split_axis=0, concat_axis=0, tiled=True)


def along_z(block):
    size = lax.axis_size("band")
    groups = [list(range(place, size, PLANE)) for place in range(PLANE)]
    return lax.all_to_all(
        block, "band", split_axis=0, concat_axis=0, tiled=True, axis_index_groups=groups
    )


def in_planes(array):
    return array.reshape((-1, PLANE) + array.shape[1:])


def by_distance(array):
    place = lax.axis_index("band") % PLANE
    return [
        lax.dynamic_index_in_dim(array, place ^ step, axis=1, keepdims=False)
        for step in range(PLANE)
    ]


def within_plane(array):
    size = lax.axis_size("band")
    pieces = by_distance(array)
    for step in range(1, PLANE):
        route = [(i, i ^ step) for i in range(size)]
        pieces[step] = lax.ppermute(pieces[step], "band", route)
    return jnp.stack(pieces, axis=1)


def across_tm(array, x_step, y_step):
    size = lax.axis_size("tm")
    ring = size // 2
    route = [
        (i, ((i // ring + y_step) % 2) * ring + (i % ring + x_step) % ring) for i in range(size)
    ]
    return lax.ppermute(array, "tm", route)


def own_row(block):
    return (
        across_tm(block, 1, 0),
        across_tm(block, -1, 0),
        across_tm(block, 0, 1),
        across_tm(block, 2, 0),
    )


def whole_table(block, left, right, across, far):
    across_left = across_tm(across, 1, 0)
    across_right = across_tm(across, -1, 0)
    across_far = across_tm(far, 0, 1)
    size = lax.axis_size("tm")
    ring = size // 2
    me = lax.axis_index("tm")
    y, x = me // ring, me % ring
    table = jnp.broadcast_to(block[None], (size,) + block.shape)
    for piece, dx, dy in (
        (left, -1, 0), (right, 1, 0), (across, 0, 1), (far, 2, 0),
        (across_left, -1, 1), (across_right, 1, 1), (across_far, 2, 1),
    ):
        at = ((y + dy) % 2) * ring + (x + dx + ring) % ring
        table = lax.dynamic_update_slice(table, piece[None], (at,) + (0,) * block.ndim)
    return table


def with_quadrature(samples):
    return jnp.stack([samples, jnp.stack([samples[:, :, 1], -samples[:, :, 0]], axis=2)])


def beam_form_of_pairs(samples, weights):
    products = jnp.einsum(
        "fkce,tkdbe->tbkdcf", samples, weights, preferred_element_type=jnp.float32
    )
    real_part = products[:, :, :, 0, 0] + products[:, :, :, 1, 1]
    imag_part = products[:, :, :, 0, 1] - products[:, :, :, 1, 0]
    return to_messages(jnp.stack([real_part, imag_part], axis=3))


def to_messages(products):
    spectra = products.astype(jnp.bfloat16)
    size = lax.axis_size("band")
    spectra = spectra.reshape((size, -1) + spectra.shape[2:])
    return jnp.transpose(spectra, (0, 2, 3, 1, 4))


def beam_form(samples, weights):
    products = jnp.einsum(
        "pfkce,tkcbe->tbkpf", samples, weights, preferred_element_type=jnp.float32
    )
    return to_messages(products)


def shards(samples, weights, prototype):
    hop_size = M // 2
    blocks = jnp.transpose(weights, (0, 1, 3, 2))
    size = lax.axis_size("tm")
    head = blocks[:HEAD]
    head = exchanged(jnp.broadcast_to(head[None], (size,) + head.shape), "tm")
    row = own_row(blocks[HEAD:])
    message = beam_form_of_pairs(samples[:, :HEAD], head)
    head_spectra = along_z(in_planes(message))
    samples, row, block, _ = lax.optimization_barrier((samples, row, blocks[HEAD:], message))
    rest = whole_table(block, *row)
    rest_message = beam_form(with_quadrature(samples[:, HEAD:]), rest)
    rest_spectra = exchanged(rest_message, "band")
    head_spectra = within_plane(head_spectra).reshape(message.shape)

    table = synth_table(prototype)
    table = table.reshape((lax.axis_size("band"), -1) + table.shape[1:])

    frame_total = samples.shape[0]
    beams = head_spectra.shape[3]
    lags = prototype.shape[0] // hop_size

    def synthesize(spectra, part):
        return jnp.einsum(
            "skcbf,skcm->bfm", spectra, part, preferred_element_type=jnp.float32
        )

    def spill_of(tail):
        tail = tail.reshape(beams, lags - 1, lags, hop_size)
        rows = []
        for row in range(lags - 1):
            rows.append(
                sum(tail[:, lags - 1 + row - lag, lag] for lag in range(row + 1, lags))
            )
        return jnp.stack(rows)

    head_table = jnp.stack(by_distance(in_planes(table[:, :HEAD])), axis=1)
    head_table = head_table.reshape(table[:, :HEAD].shape)
    base = intersection_add(synthesize(head_spectra, head_table), hop_size)
    base, spill = base[:, :frame_total], base[:, frame_total:]
    base, spill, rest_spectra = lax.optimization_barrier((base, spill, rest_spectra))
    rest_frames = synthesize(rest_spectra, table[:, HEAD:])
    spill = spill_of(rest_frames[:, frame_total - lags + 1 :]) + jnp.transpose(spill, (1, 0, 2))
    spill = spill.reshape(lags - 1, beams, -1, LANES)
    spill = jnp.transpose(spill, (0, 2, 1, 3)).reshape(-1, LANES)
    prev_tail = passed_along(spill, "tm", 1)
    out = overlapped(rest_frames, base)
    out = lax.dynamic_update_slice(out, out[: prev_tail.shape[0]] + prev_tail, (0, 0))
    out = out.reshape(-1, beams, LANES)
    return jnp.transpose(out, (1, 0, 2)).reshape(beams, frame_total * hop_size)


def solution(mesh):
    in_specs = (P("tm", "band", None, None), P("band", None, None, "tm"), P())
    out_specs = P("band", "tm")

    return jax.shard_map(shards, mesh=mesh, in_specs=in_specs, out_specs=out_specs, check_vma=False)
```

```python
import math

import jax
import jax.numpy as jnp
from jax import lax
from jax.experimental import pallas as pl
from jax.experimental.pallas import tpu as pltpu
from jax.sharding import PartitionSpec as P


M = 512
K = 256
FIRST_BIN = 32
LANES = 128
PARTS = 4
PLANE = 4
HEAD = 1


def passed_along(block, axis, distance):
    devices = range(lax.axis_size(axis))
    route = [(i - distance, i) for i in devices if i - distance in devices]
    return lax.ppermute(block, axis, route)


def synth_table(prototype):
    length = prototype.shape[0]
    bin_index = jnp.arange(K, dtype=jnp.int32) + FIRST_BIN
    tap_index = jnp.arange(length, dtype=jnp.int32)
    phase_index = bin_index[:, None] * tap_index[None, :] % M
    angles = phase_index.astype(jnp.float32) * (2.0 * math.pi / M)
    scaled = prototype[None, :] / math.sqrt(K)
    window_table = jnp.stack([jnp.cos(angles) * scaled, -jnp.sin(angles) * scaled], axis=1)
    return window_table.astype(jnp.bfloat16)


def intersection_add(frames, hop_size):
    pieces = frames.shape[-1] // hop_size
    pieces_view = frames.reshape(frames.shape[:-1] + (pieces, hop_size))
    leading = [(0, 0)] * (pieces_view.ndim - 3)
    intersection = jnp.zeros(
        pieces_view.shape[:-3] + (pieces_view.shape[-3] + pieces - 1, hop_size), frames.dtype
    )
    for lag in range(pieces):
        intersection = intersection + jnp.pad(
            pieces_view[..., lag, :], leading + [(lag, pieces - 1 - lag), (0, 0)]
        )
    return intersection


def overlap_kernel(frames_ref, base_ref, out_ref, done_ref, sems):
    beams, rows, hop_size = base_ref.shape
    lags = frames_ref.shape[2] // hop_size
    step, lanes = 32, out_ref.shape[1]
    halves = hop_size // lanes
    part = rows // PARTS

    def copy_of(index):
        span = pl.ds(index * part * halves * beams, part * halves * beams)
        return pltpu.make_async_copy(done_ref.at[span], out_ref.at[span], sems.at[index])

    for index in range(PARTS):

        def one_beam(b, carry):
            for at in range(index * part, (index + 1) * part, step):
                total = base_ref[b, pl.ds(at, step), :] + frames_ref[b, pl.ds(at, step), :hop_size]
                for lag in range(1, lags):
                    columns = pl.ds(lag * hop_size, hop_size)
                    if at:
                        total += frames_ref[b, pl.ds(at - lag, step), columns]
                    else:
                        piece = pltpu.roll(frames_ref[b, pl.ds(0, step), columns], lag, 0)
                        row = lax.broadcasted_iota(jnp.int32, piece.shape, 0)
                        total += jnp.where(row < lag, 0.0, piece)
                for half in range(halves):
                    rows_of = pl.ds((at * halves + half) * beams + b, step, stride=halves * beams)
                    done_ref[rows_of, :] = total[:, half * lanes : (half + 1) * lanes]
            return carry

        lax.fori_loop(0, beams, one_beam, 0)
        copy_of(index).start()
    for index in range(PARTS):
        copy_of(index).wait()


def overlapped(frames, base):
    beams, rows, hop_size = base.shape
    lags = frames.shape[2] // hop_size
    whole = pl.BlockSpec(memory_space=pltpu.VMEM)
    shape = (rows * hop_size // LANES * beams, LANES)
    return pl.pallas_call(
        overlap_kernel,
        out_shape=jax.ShapeDtypeStruct(shape, jnp.float32),
        in_specs=[whole, whole],
        out_specs=pl.BlockSpec(memory_space=pl.ANY),
        scratch_shapes=[pltpu.VMEM(shape, jnp.float32), pltpu.SemaphoreType.DMA((PARTS,))],
        cost_estimate=pl.CostEstimate(
            flops=beams * lags * rows * hop_size,
            bytes_accessed=4 * beams * (lags + 2) * rows * hop_size,
            transcendentals=0,
        ),
        compiler_params=pltpu.CompilerParams(vmem_limit_bytes=20 * 2**20),
        name="overlap",
    )(frames, base)


def exchanged(block, axis):
    return lax.all_to_all(block, axis, split_axis=0, concat_axis=0, tiled=True)


def along_z(block):
    size = lax.axis_size("band")
    groups = [list(range(place, size, PLANE)) for place in range(PLANE)]
    return lax.all_to_all(
        block, "band", split_axis=0, concat_axis=0, tiled=True, axis_index_groups=groups
    )


def in_planes(array):
    return array.reshape((-1, PLANE) + array.shape[1:])


def by_distance(array):
    place = lax.axis_index("band") % PLANE
    return [
        lax.dynamic_index_in_dim(array, place ^ step, axis=1, keepdims=False)
        for step in range(PLANE)
    ]


def within_plane(array):
    size = lax.axis_size("band")
    pieces = by_distance(array)
    for step in range(1, PLANE):
        route = [(i, i ^ step) for i in range(size)]
        pieces[step] = lax.ppermute(pieces[step], "band", route)
    return jnp.stack(pieces, axis=1)


def across_tm(array, x_step, y_step):
    size = lax.axis_size("tm")
    ring = size // 2
    route = [
        (i, ((i // ring + y_step) % 2) * ring + (i % ring + x_step) % ring) for i in range(size)
    ]
    return lax.ppermute(array, "tm", route)


def own_row(block):
    across, far = across_tm(block, 0, 1), across_tm(block, 2, 0)
    left, right = across_tm(block, 1, 0), across_tm(block, -1, 0)
    return left, right, across, far


def whole_table(block, left, right, across, far):
    across_left = across_tm(across, 1, 0)
    across_right = across_tm(across, -1, 0)
    across_far = across_tm(far, 0, 1)
    size = lax.axis_size("tm")
    ring = size // 2
    me = lax.axis_index("tm")
    y, x = me // ring, me % ring
    table = jnp.broadcast_to(block[None], (size,) + block.shape)
    for piece, dx, dy in (
        (across, 0, 1), (far, 2, 0), (across_left, -1, 1),
        (left, -1, 0), (right, 1, 0),
        (across_right, 1, 1), (across_far, 2, 1),
    ):
        at = ((y + dy) % 2) * ring + (x + dx + ring) % ring
        table = lax.dynamic_update_slice(table, piece[None], (at,) + (0,) * block.ndim)
    return table


def with_quadrature(samples):
    return jnp.stack([samples, jnp.stack([samples[:, :, 1], -samples[:, :, 0]], axis=2)])


def beam_form_of_pairs(samples, weights):
    products = jnp.einsum(
        "fkce,tkdbe->tbkdcf", samples, weights, preferred_element_type=jnp.float32
    )
    real_part = products[:, :, :, 0, 0] + products[:, :, :, 1, 1]
    imag_part = products[:, :, :, 0, 1] - products[:, :, :, 1, 0]
    return to_messages(jnp.stack([real_part, imag_part], axis=3))


def to_messages(products):
    spectra = products.astype(jnp.bfloat16)
    size = lax.axis_size("band")
    spectra = spectra.reshape((size, -1) + spectra.shape[2:])
    return jnp.transpose(spectra, (0, 2, 3, 1, 4))


def beam_form(samples, weights):
    products = jnp.einsum(
        "pfkce,tkcbe->tbkpf", samples, weights, preferred_element_type=jnp.float32
    )
    return to_messages(products)


def shards(samples, weights, prototype):
    hop_size = M // 2
    blocks = jnp.transpose(weights, (0, 1, 3, 2))
    size = lax.axis_size("tm")
    head = blocks[:HEAD]
    head = exchanged(jnp.broadcast_to(head[None], (size,) + head.shape), "tm")
    left, right, across, far = own_row(blocks[HEAD:])
    message = beam_form_of_pairs(samples[:, :HEAD], head)
    head_spectra = along_z(in_planes(message))
    samples, across, far, block, _ = lax.optimization_barrier(
        (samples, across, far, blocks[HEAD:], message)
    )
    rest = whole_table(block, left, right, across, far)
    rest_message = beam_form(with_quadrature(samples[:, HEAD:]), rest)
    rest_spectra = exchanged(rest_message, "band")
    head_spectra = within_plane(head_spectra).reshape(message.shape)

    table = synth_table(prototype)
    table = table.reshape((lax.axis_size("band"), -1) + table.shape[1:])

    frame_total = samples.shape[0]
    beams = head_spectra.shape[3]
    lags = prototype.shape[0] // hop_size

    def synthesize(spectra, part):
        return jnp.einsum(
            "skcbf,skcm->bfm", spectra, part, preferred_element_type=jnp.float32
        )

    def spill_of(tail):
        tail = tail.reshape(beams, lags - 1, lags, hop_size)
        rows = []
        for row in range(lags - 1):
            rows.append(
                sum(tail[:, lags - 1 + row - lag, lag] for lag in range(row + 1, lags))
            )
        return jnp.stack(rows)

    head_table = jnp.stack(by_distance(in_planes(table[:, :HEAD])), axis=1)
    head_table = head_table.reshape(table[:, :HEAD].shape)
    base = intersection_add(synthesize(head_spectra, head_table), hop_size)
    base, spill = base[:, :frame_total], base[:, frame_total:]
    base, spill, rest_spectra = lax.optimization_barrier((base, spill, rest_spectra))
    rest_frames = synthesize(rest_spectra, table[:, HEAD:])
    spill = spill_of(rest_frames[:, frame_total - lags + 1 :]) + jnp.transpose(spill, (1, 0, 2))
    spill = spill.reshape(lags - 1, beams, -1, LANES)
    spill = jnp.transpose(spill, (0, 2, 1, 3)).reshape(-1, LANES)
    prev_tail = passed_along(spill, "tm", 1)
    out = overlapped(rest_frames, base)
    out = lax.dynamic_update_slice(out, out[: prev_tail.shape[0]] + prev_tail, (0, 0))
    out = out.reshape(-1, beams, LANES)
    return jnp.transpose(out, (1, 0, 2)).reshape(beams, frame_total * hop_size)


def solution(mesh):
    in_specs = (P("tm", "band", None, None), P("band", None, None, "tm"), P())
    out_specs = P("band", "tm")

    return jax.shard_map(shards, mesh=mesh, in_specs=in_specs, out_specs=out_specs, check_vma=False)
```

```python
import math

import jax
import jax.numpy as jnp
from jax import lax
from jax.experimental import pallas as pl
from jax.experimental.pallas import tpu as pltpu
from jax.sharding import PartitionSpec as P


M = 512
K = 256
FIRST_BIN = 32
LANES = 128
PARTS = 4
PLANE = 4
HEAD = 1


def passed_along(block, axis, distance):
    devices = range(lax.axis_size(axis))
    route = [(i - distance, i) for i in devices if i - distance in devices]
    return lax.ppermute(block, axis, route)


def synth_table(prototype):
    length = prototype.shape[0]
    bin_index = jnp.arange(K, dtype=jnp.int32) + FIRST_BIN
    tap_index = jnp.arange(length, dtype=jnp.int32)
    phase_index = bin_index[:, None] * tap_index[None, :] % M
    angles = phase_index.astype(jnp.float32) * (2.0 * math.pi / M)
    scaled = prototype[None, :] / math.sqrt(K)
    window_table = jnp.stack([jnp.cos(angles) * scaled, -jnp.sin(angles) * scaled], axis=1)
    return window_table.astype(jnp.bfloat16)


def intersection_add(frames, hop_size):
    pieces = frames.shape[-1] // hop_size
    pieces_view = frames.reshape(frames.shape[:-1] + (pieces, hop_size))
    leading = [(0, 0)] * (pieces_view.ndim - 3)
    intersection = jnp.zeros(
        pieces_view.shape[:-3] + (pieces_view.shape[-3] + pieces - 1, hop_size), frames.dtype
    )
    for lag in range(pieces):
        intersection = intersection + jnp.pad(
            pieces_view[..., lag, :], leading + [(lag, pieces - 1 - lag), (0, 0)]
        )
    return intersection


def overlap_kernel(frames_ref, base_ref, out_ref, done_ref, sems):
    beams, rows, hop_size = base_ref.shape
    lags = frames_ref.shape[2] // hop_size
    step, lanes = 32, out_ref.shape[1]
    halves = hop_size // lanes
    part = rows // PARTS

    def copy_of(index):
        span = pl.ds(index * part * halves * beams, part * halves * beams)
        return pltpu.make_async_copy(done_ref.at[span], out_ref.at[span], sems.at[index])

    for index in range(PARTS):

        def one_beam(b, carry):
            for at in range(index * part, (index + 1) * part, step):
                total = base_ref[b, pl.ds(at, step), :] + frames_ref[b, pl.ds(at, step), :hop_size]
                for lag in range(1, lags):
                    columns = pl.ds(lag * hop_size, hop_size)
                    if at:
                        total += frames_ref[b, pl.ds(at - lag, step), columns]
                    else:
                        piece = pltpu.roll(frames_ref[b, pl.ds(0, step), columns], lag, 0)
                        row = lax.broadcasted_iota(jnp.int32, piece.shape, 0)
                        total += jnp.where(row < lag, 0.0, piece)
                for half in range(halves):
                    rows_of = pl.ds((at * halves + half) * beams + b, step, stride=halves * beams)
                    done_ref[rows_of, :] = total[:, half * lanes : (half + 1) * lanes]
            return carry

        lax.fori_loop(0, beams, one_beam, 0)
        copy_of(index).start()
    for index in range(PARTS):
        copy_of(index).wait()


def overlapped(frames, base):
    beams, rows, hop_size = base.shape
    lags = frames.shape[2] // hop_size
    whole = pl.BlockSpec(memory_space=pltpu.VMEM)
    shape = (rows * hop_size // LANES * beams, LANES)
    return pl.pallas_call(
        overlap_kernel,
        out_shape=jax.ShapeDtypeStruct(shape, jnp.float32),
        in_specs=[whole, whole],
        out_specs=pl.BlockSpec(memory_space=pl.ANY),
        scratch_shapes=[pltpu.VMEM(shape, jnp.float32), pltpu.SemaphoreType.DMA((PARTS,))],
        cost_estimate=pl.CostEstimate(
            flops=beams * lags * rows * hop_size,
            bytes_accessed=4 * beams * (lags + 2) * rows * hop_size,
            transcendentals=0,
        ),
        compiler_params=pltpu.CompilerParams(vmem_limit_bytes=20 * 2**20),
        name="overlap",
    )(frames, base)


def exchanged(block, axis):
    return lax.all_to_all(block, axis, split_axis=0, concat_axis=0, tiled=True)


def along_z(block):
    size = lax.axis_size("band")
    groups = [list(range(place, size, PLANE)) for place in range(PLANE)]
    return lax.all_to_all(
        block, "band", split_axis=0, concat_axis=0, tiled=True, axis_index_groups=groups
    )


def in_planes(array):
    return array.reshape((-1, PLANE) + array.shape[1:])


def by_distance(array):
    place = lax.axis_index("band") % PLANE
    return [
        lax.dynamic_index_in_dim(array, place ^ step, axis=1, keepdims=False)
        for step in range(PLANE)
    ]


def within_plane(array):
    size = lax.axis_size("band")
    pieces = by_distance(array)
    for step in range(1, PLANE):
        route = [(i, i ^ step) for i in range(size)]
        pieces[step] = lax.ppermute(pieces[step], "band", route)
    return jnp.stack(pieces, axis=1)


def across_tm(array, x_step, y_step):
    size = lax.axis_size("tm")
    ring = size // 2
    route = [
        (i, ((i // ring + y_step) % 2) * ring + (i % ring + x_step) % ring) for i in range(size)
    ]
    return lax.ppermute(array, "tm", route)


def own_row(block):
    across = across_tm(block, 0, 1)
    left, right = across_tm(block, 1, 0), across_tm(block, -1, 0)
    far = across_tm(block, 2, 0)
    return left, right, across, far


def whole_table(block, left, right, across, far):
    across_left = across_tm(across, 1, 0)
    across_right = across_tm(across, -1, 0)
    far, block = lax.optimization_barrier((far, block))
    across_far = across_tm(far, 0, 1)
    size = lax.axis_size("tm")
    ring = size // 2
    me = lax.axis_index("tm")
    y, x = me // ring, me % ring
    table = jnp.broadcast_to(block[None], (size,) + block.shape)
    for piece, dx, dy in (
        (across, 0, 1), (far, 2, 0), (across_left, -1, 1),
        (left, -1, 0), (right, 1, 0),
        (across_right, 1, 1), (across_far, 2, 1),
    ):
        at = ((y + dy) % 2) * ring + (x + dx + ring) % ring
        table = lax.dynamic_update_slice(table, piece[None], (at,) + (0,) * block.ndim)
    return table


def with_quadrature(samples):
    return jnp.stack([samples, jnp.stack([samples[:, :, 1], -samples[:, :, 0]], axis=2)])


def beam_form_of_pairs(samples, weights):
    products = jnp.einsum(
        "fkce,tkdbe->tbkdcf", samples, weights, preferred_element_type=jnp.float32
    )
    real_part = products[:, :, :, 0, 0] + products[:, :, :, 1, 1]
    imag_part = products[:, :, :, 0, 1] - products[:, :, :, 1, 0]
    return to_messages(jnp.stack([real_part, imag_part], axis=3))


def to_messages(products):
    spectra = products.astype(jnp.bfloat16)
    size = lax.axis_size("band")
    spectra = spectra.reshape((size, -1) + spectra.shape[2:])
    return jnp.transpose(spectra, (0, 2, 3, 1, 4))


def beam_form(samples, weights):
    products = jnp.einsum(
        "pfkce,tkcbe->tbkpf", samples, weights, preferred_element_type=jnp.float32
    )
    return to_messages(products)


def shards(samples, weights, prototype):
    hop_size = M // 2
    blocks = jnp.transpose(weights, (0, 1, 3, 2))
    size = lax.axis_size("tm")
    head = blocks[:HEAD]
    head = exchanged(jnp.broadcast_to(head[None], (size,) + head.shape), "tm")
    left, right, across, far = own_row(blocks[HEAD:])
    message = beam_form_of_pairs(samples[:, :HEAD], head)
    head_spectra = along_z(in_planes(message))
    samples, across, block, _ = lax.optimization_barrier(
        (samples, across, blocks[HEAD:], message)
    )
    rest = whole_table(block, left, right, across, far)
    rest_message = beam_form(with_quadrature(samples[:, HEAD:]), rest)
    rest_spectra = exchanged(rest_message, "band")
    head_spectra = within_plane(head_spectra).reshape(message.shape)

    table = synth_table(prototype)
    table = table.reshape((lax.axis_size("band"), -1) + table.shape[1:])

    frame_total = samples.shape[0]
    beams = head_spectra.shape[3]
    lags = prototype.shape[0] // hop_size

    def synthesize(spectra, part):
        return jnp.einsum(
            "skcbf,skcm->bfm", spectra, part, preferred_element_type=jnp.float32
        )

    def spill_of(tail):
        tail = tail.reshape(beams, lags - 1, lags, hop_size)
        rows = []
        for row in range(lags - 1):
            rows.append(
                sum(tail[:, lags - 1 + row - lag, lag] for lag in range(row + 1, lags))
            )
        return jnp.stack(rows)

    head_table = jnp.stack(by_distance(in_planes(table[:, :HEAD])), axis=1)
    head_table = head_table.reshape(table[:, :HEAD].shape)
    base = intersection_add(synthesize(head_spectra, head_table), hop_size)
    base, spill = base[:, :frame_total], base[:, frame_total:]
    base, spill, rest_spectra = lax.optimization_barrier((base, spill, rest_spectra))
    rest_frames = synthesize(rest_spectra, table[:, HEAD:])
    spill = spill_of(rest_frames[:, frame_total - lags + 1 :]) + jnp.transpose(spill, (1, 0, 2))
    spill = spill.reshape(lags - 1, beams, -1, LANES)
    spill = jnp.transpose(spill, (0, 2, 1, 3)).reshape(-1, LANES)
    prev_tail = passed_along(spill, "tm", 1)
    out = overlapped(rest_frames, base)
    out = lax.dynamic_update_slice(out, out[: prev_tail.shape[0]] + prev_tail, (0, 0))
    out = out.reshape(-1, beams, LANES)
    return jnp.transpose(out, (1, 0, 2)).reshape(beams, frame_total * hop_size)


def solution(mesh):
    in_specs = (P("tm", "band", None, None), P("band", None, None, "tm"), P())
    out_specs = P("band", "tm")

    return jax.shard_map(shards, mesh=mesh, in_specs=in_specs, out_specs=out_specs, check_vma=False)
```

```python
import math

import jax
import jax.numpy as jnp
from jax import lax
from jax.experimental import pallas as pl
from jax.experimental.pallas import tpu as pltpu
from jax.sharding import PartitionSpec as P


M = 512
K = 256
FIRST_BIN = 32
LANES = 128
PARTS = 4
PLANE = 4
HEAD = 1


def passed_along(block, axis, distance):
    devices = range(lax.axis_size(axis))
    route = [(i - distance, i) for i in devices if i - distance in devices]
    return lax.ppermute(block, axis, route)


def synth_table(prototype):
    length = prototype.shape[0]
    bin_index = jnp.arange(K, dtype=jnp.int32) + FIRST_BIN
    tap_index = jnp.arange(length, dtype=jnp.int32)
    phase_index = bin_index[:, None] * tap_index[None, :] % M
    angles = phase_index.astype(jnp.float32) * (2.0 * math.pi / M)
    scaled = prototype[None, :] / math.sqrt(K)
    window_table = jnp.stack([jnp.cos(angles) * scaled, -jnp.sin(angles) * scaled], axis=1)
    return window_table.astype(jnp.bfloat16)


def intersection_add(frames, hop_size):
    pieces = frames.shape[-1] // hop_size
    pieces_view = frames.reshape(frames.shape[:-1] + (pieces, hop_size))
    leading = [(0, 0)] * (pieces_view.ndim - 3)
    intersection = jnp.zeros(
        pieces_view.shape[:-3] + (pieces_view.shape[-3] + pieces - 1, hop_size), frames.dtype
    )
    for lag in range(pieces):
        intersection = intersection + jnp.pad(
            pieces_view[..., lag, :], leading + [(lag, pieces - 1 - lag), (0, 0)]
        )
    return intersection


def overlap_kernel(frames_ref, base_ref, out_ref, done_ref, sems):
    beams, rows, hop_size = base_ref.shape
    lags = frames_ref.shape[2] // hop_size
    step, lanes = 32, out_ref.shape[1]
    halves = hop_size // lanes
    part = rows // PARTS

    def copy_of(index):
        span = pl.ds(index * part * halves * beams, part * halves * beams)
        return pltpu.make_async_copy(done_ref.at[span], out_ref.at[span], sems.at[index])

    for index in range(PARTS):

        def one_beam(b, carry):
            for at in range(index * part, (index + 1) * part, step):
                total = base_ref[b, pl.ds(at, step), :] + frames_ref[b, pl.ds(at, step), :hop_size]
                for lag in range(1, lags):
                    columns = pl.ds(lag * hop_size, hop_size)
                    if at:
                        total += frames_ref[b, pl.ds(at - lag, step), columns]
                    else:
                        piece = pltpu.roll(frames_ref[b, pl.ds(0, step), columns], lag, 0)
                        row = lax.broadcasted_iota(jnp.int32, piece.shape, 0)
                        total += jnp.where(row < lag, 0.0, piece)
                for half in range(halves):
                    rows_of = pl.ds((at * halves + half) * beams + b, step, stride=halves * beams)
                    done_ref[rows_of, :] = total[:, half * lanes : (half + 1) * lanes]
            return carry

        lax.fori_loop(0, beams, one_beam, 0)
        copy_of(index).start()
    for index in range(PARTS):
        copy_of(index).wait()


def overlapped(frames, base):
    beams, rows, hop_size = base.shape
    lags = frames.shape[2] // hop_size
    whole = pl.BlockSpec(memory_space=pltpu.VMEM)
    shape = (rows * hop_size // LANES * beams, LANES)
    return pl.pallas_call(
        overlap_kernel,
        out_shape=jax.ShapeDtypeStruct(shape, jnp.float32),
        in_specs=[whole, whole],
        out_specs=pl.BlockSpec(memory_space=pl.ANY),
        scratch_shapes=[pltpu.VMEM(shape, jnp.float32), pltpu.SemaphoreType.DMA((PARTS,))],
        cost_estimate=pl.CostEstimate(
            flops=beams * lags * rows * hop_size,
            bytes_accessed=4 * beams * (lags + 2) * rows * hop_size,
            transcendentals=0,
        ),
        compiler_params=pltpu.CompilerParams(vmem_limit_bytes=20 * 2**20),
        name="overlap",
    )(frames, base)


def exchanged(block, axis):
    return lax.all_to_all(block, axis, split_axis=0, concat_axis=0, tiled=True)


def along_z(block):
    size = lax.axis_size("band")
    groups = [list(range(place, size, PLANE)) for place in range(PLANE)]
    return lax.all_to_all(
        block, "band", split_axis=0, concat_axis=0, tiled=True, axis_index_groups=groups
    )


def in_planes(array):
    return array.reshape((-1, PLANE) + array.shape[1:])


def by_distance(array):
    place = lax.axis_index("band") % PLANE
    return [
        lax.dynamic_index_in_dim(array, place ^ step, axis=1, keepdims=False)
        for step in range(PLANE)
    ]


def within_plane(array):
    size = lax.axis_size("band")
    pieces = by_distance(array)
    for step in range(1, PLANE):
        route = [(i, i ^ step) for i in range(size)]
        pieces[step] = lax.ppermute(pieces[step], "band", route)
    return jnp.stack(pieces, axis=1)


def across_tm(array, x_step, y_step):
    size = lax.axis_size("tm")
    ring = size // 2
    route = [
        (i, ((i // ring + y_step) % 2) * ring + (i % ring + x_step) % ring) for i in range(size)
    ]
    return lax.ppermute(array, "tm", route)


def own_row(block):
    across = across_tm(block, 0, 1)
    left = across_tm(block, 1, 0)
    far = across_tm(block, 2, 0)
    return left, across, far


def whole_table(block, left, across, far):
    across_left = across_tm(across, 1, 0)
    across_right = across_tm(across, -1, 0)
    far, block = lax.optimization_barrier((far, block))
    across_far = across_tm(far, 0, 1)
    right = across_tm(block, -1, 0)
    size = lax.axis_size("tm")
    ring = size // 2
    me = lax.axis_index("tm")
    y, x = me // ring, me % ring
    table = jnp.broadcast_to(block[None], (size,) + block.shape)
    for piece, dx, dy in (
        (across, 0, 1), (far, 2, 0), (across_left, -1, 1),
        (left, -1, 0), (right, 1, 0),
        (across_right, 1, 1), (across_far, 2, 1),
    ):
        at = ((y + dy) % 2) * ring + (x + dx + ring) % ring
        table = lax.dynamic_update_slice(table, piece[None], (at,) + (0,) * block.ndim)
    return table


def with_quadrature(samples):
    return jnp.stack([samples, jnp.stack([samples[:, :, 1], -samples[:, :, 0]], axis=2)])


def beam_form_of_pairs(samples, weights):
    products = jnp.einsum(
        "fkce,tkdbe->tbkdcf", samples, weights, preferred_element_type=jnp.float32
    )
    real_part = products[:, :, :, 0, 0] + products[:, :, :, 1, 1]
    imag_part = products[:, :, :, 0, 1] - products[:, :, :, 1, 0]
    return to_messages(jnp.stack([real_part, imag_part], axis=3))


def to_messages(products):
    spectra = products.astype(jnp.bfloat16)
    size = lax.axis_size("band")
    spectra = spectra.reshape((size, -1) + spectra.shape[2:])
    return jnp.transpose(spectra, (0, 2, 3, 1, 4))


def beam_form(samples, weights):
    products = jnp.einsum(
        "pfkce,tkcbe->tbkpf", samples, weights, preferred_element_type=jnp.float32
    )
    return to_messages(products)


def shards(samples, weights, prototype):
    hop_size = M // 2
    blocks = jnp.transpose(weights, (0, 1, 3, 2))
    size = lax.axis_size("tm")
    head = blocks[:HEAD]
    head = exchanged(jnp.broadcast_to(head[None], (size,) + head.shape), "tm")
    left, across, far = own_row(blocks[HEAD:])
    message = beam_form_of_pairs(samples[:, :HEAD], head)
    head_spectra = along_z(in_planes(message))
    samples, across, block, _ = lax.optimization_barrier(
        (samples, across, blocks[HEAD:], message)
    )
    rest = whole_table(block, left, across, far)
    rest_message = beam_form(with_quadrature(samples[:, HEAD:]), rest)
    rest_spectra = exchanged(rest_message, "band")
    head_spectra = within_plane(head_spectra).reshape(message.shape)

    table = synth_table(prototype)
    table = table.reshape((lax.axis_size("band"), -1) + table.shape[1:])

    frame_total = samples.shape[0]
    beams = head_spectra.shape[3]
    lags = prototype.shape[0] // hop_size

    def synthesize(spectra, part):
        return jnp.einsum(
            "skcbf,skcm->bfm", spectra, part, preferred_element_type=jnp.float32
        )

    def spill_of(tail):
        tail = tail.reshape(beams, lags - 1, lags, hop_size)
        rows = []
        for row in range(lags - 1):
            rows.append(
                sum(tail[:, lags - 1 + row - lag, lag] for lag in range(row + 1, lags))
            )
        return jnp.stack(rows)

    head_table = jnp.stack(by_distance(in_planes(table[:, :HEAD])), axis=1)
    head_table = head_table.reshape(table[:, :HEAD].shape)
    base = intersection_add(synthesize(head_spectra, head_table), hop_size)
    base, spill = base[:, :frame_total], base[:, frame_total:]
    base, spill, rest_spectra = lax.optimization_barrier((base, spill, rest_spectra))
    rest_frames = synthesize(rest_spectra, table[:, HEAD:])
    spill = spill_of(rest_frames[:, frame_total - lags + 1 :]) + jnp.transpose(spill, (1, 0, 2))
    spill = spill.reshape(lags - 1, beams, -1, LANES)
    spill = jnp.transpose(spill, (0, 2, 1, 3)).reshape(-1, LANES)
    prev_tail = passed_along(spill, "tm", 1)
    out = overlapped(rest_frames, base)
    out = lax.dynamic_update_slice(out, out[: prev_tail.shape[0]] + prev_tail, (0, 0))
    out = out.reshape(-1, beams, LANES)
    return jnp.transpose(out, (1, 0, 2)).reshape(beams, frame_total * hop_size)


def solution(mesh):
    in_specs = (P("tm", "band", None, None), P("band", None, None, "tm"), P())
    out_specs = P("band", "tm")

    return jax.shard_map(shards, mesh=mesh, in_specs=in_specs, out_specs=out_specs, check_vma=False)
```
